32 devices in a mesh: obj: 8 (over z, x), view: 4 (over y, core).
Axes of the slice: x: 2, y: 2, z: 4, core: 2. Of those that a mesh axis runs over, the one named last changes fastest.
Arguments:
- features: bfloat16 [8, 4, 1369, 1024], P('obj', 'view'), may hold values from -6 to 6
- projection: int32 [8, 4, 1369], P('obj'), may hold values from 0 to 511, as said below
- active_count: int32 [8], P('obj'), may hold values from 256 to 512, as said below
- in_weight: bfloat16 [1024, 768], replicated, may hold values from -0.1875 to 0.1875
- norm_gain: float32 [768], replicated, may hold values from 0.1 to 1.9
- qkv_weight: bfloat16 [768, 2304], replicated, may hold values from -4 to 4
- out_weight: bfloat16 [768, 768], replicated, may hold values from -0.21875 to 0.21875
- cotangent: bfloat16 [8, 512, 768], P('obj', 'view'), may hold values from -6 to 6
Outputs:
- latent: bfloat16 [8, 512, 768], P('obj', 'view')
- in_grad: float32 [1024, 768], P('view')
- qkv_grad: float32 [768, 2304], P('view')
- out_grad: float32 [768, 768], P('view')
The draws below stay inside these ranges and needn't reach their ends.
Inputs may be any that keep to these rules, and one draw needn't show every extreme that they name: `projection`: every entry is below its object's active_count; in every object some live slots receive no patch. `active_count`: slots from this number on are empty: they are no keys, and their rows of latent are zero.
All inputs are finite; a program needn't handle non-finite values.
Results may differ from the reference program's by a relative error of at most 0.02.
Values may be sent and summed in bfloat16 or wider, within the bound.
No kernel may reach another device: no remote copies, remote signals or barrier semaphores. Data moves between devices by JAX's collectives and lax.ppermute only.
A program may use at most 64 MiB of HBM per device.

```python
import jax
import jax.numpy as jnp
from jax import lax

FEAT = 1024
WIDTH = 768
HEADS = 12
HEAD_DIM = 64
PATCH = 1369
VOX_DEV = 128
OBJECTS = 8
VIEWS = 4
VOX = 512
N_VIEW = 4


def shared_counts(key):
    return jax.random.randint(jax.random.fold_in(key, 101), (OBJECTS,), VOX // 2, VOX + 1, dtype=jnp.int32)


def draw_active_count(key, part):
    return shared_counts(key)


def draw_projection(key, part):
    live_counts = shared_counts(key)
    offsets = jax.random.randint(jax.random.fold_in(key, 102), (OBJECTS, 1, 1), 1, 16, dtype=jnp.int32)
    ceiling = jnp.broadcast_to(live_counts[:, None, None], (OBJECTS, VIEWS, PATCH))
    chosen = jax.random.randint(jax.random.fold_in(key, 103), (OBJECTS, VIEWS, PATCH), 0, ceiling, dtype=jnp.int32)
    return jnp.where(chosen % 16 == offsets, chosen - 1, chosen).astype(jnp.int32)


def draw_qkv_weight(key, part):
    drawn = jax.random.normal(jax.random.fold_in(key, 11), (WIDTH, 3 * WIDTH), jnp.float32) * WIDTH ** (-0.5)
    return jnp.clip(drawn, -4.0, 4.0).astype(jnp.bfloat16)


def level_of(stream_key, shape, pieces, low, largest):
    factor_of = 1.0
    for position, blocks in pieces:
        draws = jax.random.uniform(jax.random.fold_in(jax.random.fold_in(stream_key, 6), position), (blocks,), jnp.float32, low / len(pieces), largest / len(pieces))
        factor_of = factor_of * jnp.repeat(jnp.exp(draws), shape[position] // blocks).reshape((-1,) + (1,) * (len(shape) - 1 - position))
    return factor_of


def noise(stream_key, extent, scale, most, shards=(), kind=jnp.bfloat16):
    drawn = scale * jax.random.normal(stream_key, extent, jnp.float32)
    if shards:
        drawn = drawn * level_of(stream_key, extent, shards, -0.22, 0.18)
    return jnp.clip(drawn, -most, most).astype(kind)


def setup_inputs(seed: int = 0) -> dict:
    arg_keys = jax.random.split(jax.random.key(seed), 9)
    features = noise(arg_keys[0], (OBJECTS, VIEWS, PATCH, FEAT), 1.0, 6.0, ((0, 8), (1, 4)))
    projection = draw_projection(jax.random.fold_in(arg_keys[8], 71), 0)
    active_count = draw_active_count(jax.random.fold_in(arg_keys[8], 71), 0)
    in_weight = noise(arg_keys[3], (FEAT, WIDTH), FEAT ** -0.5, 0.1875)
    norm_gain = jnp.clip(1.0 + 0.18 * jax.random.normal(arg_keys[4], (WIDTH,), jnp.float32), 0.1, 1.9)
    qkv_weight = draw_qkv_weight(jax.random.fold_in(arg_keys[8], 71), 0)
    out_weight = noise(arg_keys[6], (WIDTH, WIDTH), WIDTH ** -0.5, 0.21875)
    cotangent = noise(arg_keys[7], (OBJECTS, VOX, WIDTH), 1.0, 6.0, ((0, 8), (1, 4)))
    return {"features": features, "projection": projection, "active_count": active_count, "in_weight": in_weight, "norm_gain": norm_gain, "qkv_weight": qkv_weight, "out_weight": out_weight, "cotangent": cotangent}


def normalize(base_rows):
    center = lax.optimization_barrier(jnp.mean(base_rows, axis=-1, keepdims=True))
    shifted = base_rows - center
    spread = lax.optimization_barrier(jnp.mean(shifted * shifted, axis=-1, keepdims=True))
    inverse = lax.rsqrt(spread + 1e-06)
    return (shifted * inverse, inverse)

def encode_object(feat_views, proj_views, live_count, upstream, in_weight, norm_gain, qkv_weight, out_weight):
    flat_feat = feat_views.reshape(VIEWS * PATCH, FEAT).astype(jnp.float32)
    flat_proj = proj_views.reshape(VIEWS * PATCH).astype(jnp.int32)
    totals = jax.ops.segment_sum(flat_feat, flat_proj, num_segments=VOX)
    counts = jax.ops.segment_sum(jnp.ones((VIEWS * PATCH,), jnp.float32), flat_proj, num_segments=VOX)
    voxels = (totals / jnp.maximum(counts, 1.0)[:, None]).astype(jnp.bfloat16)
    slot_ids = jnp.arange(VOX, dtype=jnp.int32)
    live_rows = (slot_ids < live_count).astype(jnp.float32)
    base_rows = jnp.dot(voxels, in_weight, preferred_element_type=jnp.float32)
    unit_rows, inverse = normalize(base_rows)
    normed = (unit_rows * norm_gain).astype(jnp.bfloat16)
    packed = jnp.dot(normed, qkv_weight, preferred_element_type=jnp.float32).astype(jnp.bfloat16)
    queries = packed[:, :WIDTH].reshape(VOX, HEADS, HEAD_DIM).astype(jnp.float32)
    key_heads = packed[:, WIDTH:2 * WIDTH].reshape(VOX, HEADS, HEAD_DIM).astype(jnp.float32)
    value_heads = packed[:, 2 * WIDTH:].reshape(VOX, HEADS, HEAD_DIM).astype(jnp.float32)
    inv_root = HEAD_DIM ** (-0.5)
    scores = jnp.einsum('qhd,khd->hqk', queries, key_heads) * inv_root
    key_live = live_rows[None, None, :] > 0.5
    masked = jnp.where(key_live, scores, -1e+30)
    row_peak = lax.optimization_barrier(jnp.max(masked, axis=-1, keepdims=True))
    expo_terms = jnp.where(key_live, jnp.exp(masked - row_peak), 0.0)
    weights = expo_terms / lax.optimization_barrier(jnp.sum(expo_terms, axis=-1, keepdims=True))
    prob_rows = weights.astype(jnp.bfloat16)
    mixed_full = jnp.einsum('hqk,khd->qhd', prob_rows.astype(jnp.float32), value_heads)
    attended = mixed_full.reshape(VOX, WIDTH).astype(jnp.bfloat16)
    branch = jnp.dot(attended, out_weight, preferred_element_type=jnp.float32)
    latent = (live_rows[:, None] * (base_rows + branch)).astype(jnp.bfloat16)
    seed_rows = (upstream.astype(jnp.float32) * live_rows[:, None] * (1.0 / OBJECTS)).astype(jnp.bfloat16)
    out_grad = jnp.dot(attended.T, seed_rows, preferred_element_type=jnp.float32)
    grad_attended = jnp.dot(seed_rows, out_weight.T, preferred_element_type=jnp.float32).astype(jnp.bfloat16)
    grad_heads = grad_attended.reshape(VOX, HEADS, HEAD_DIM).astype(jnp.float32)
    grad_probs = jnp.einsum('qhd,khd->hqk', grad_heads, value_heads)
    delta_rows = lax.optimization_barrier(jnp.sum(grad_heads * mixed_full, axis=-1)).T[:, :, None]
    grad_scores = (weights * (grad_probs - delta_rows) * inv_root).astype(jnp.bfloat16)
    grad_queries = jnp.einsum('hqk,khd->qhd', grad_scores.astype(jnp.float32), key_heads).reshape(VOX, WIDTH)
    score_blocks = grad_scores.astype(jnp.float32).reshape(HEADS, N_VIEW, VOX_DEV, VOX)
    prob_blocks = prob_rows.astype(jnp.float32).reshape(HEADS, N_VIEW, VOX_DEV, VOX)
    query_blocks = queries.reshape(N_VIEW, VOX_DEV, HEADS, HEAD_DIM)
    grad_blocks = grad_heads.reshape(N_VIEW, VOX_DEV, HEADS, HEAD_DIM)
    key_parts = jnp.einsum('hbqk,bqhd->bkhd', score_blocks, query_blocks).reshape(N_VIEW, VOX, WIDTH)
    value_parts = jnp.einsum('hbqk,bqhd->bkhd', prob_blocks, grad_blocks).reshape(N_VIEW, VOX, WIDTH)
    block_parts = jnp.concatenate([key_parts, value_parts], axis=2).astype(jnp.bfloat16)
    block_parts = lax.optimization_barrier(block_parts)
    key_grads = lax.optimization_barrier(jnp.sum(block_parts.astype(jnp.float32), axis=0))
    grad_packed = jnp.concatenate([grad_queries, key_grads], axis=1).astype(jnp.bfloat16)
    qkv_grad = jnp.dot(normed.T, grad_packed, preferred_element_type=jnp.float32)
    grad_normed = jnp.dot(grad_packed, qkv_weight.T, preferred_element_type=jnp.float32)
    grad_unit = grad_normed * norm_gain
    grad_branch = inverse * (grad_unit - lax.optimization_barrier(jnp.mean(grad_unit, axis=-1, keepdims=True)) - unit_rows * lax.optimization_barrier(jnp.mean(grad_unit * unit_rows, axis=-1, keepdims=True)))
    grad_base = (seed_rows.astype(jnp.float32) + grad_branch).astype(jnp.bfloat16)
    in_grad = jnp.dot(voxels.T, grad_base, preferred_element_type=jnp.float32)
    return (latent, in_grad, qkv_grad, out_grad)

def reference(features, projection, active_count, in_weight, norm_gain, qkv_weight, out_weight, cotangent):

    def advance(running, items):
        feat_views, proj_views, live_count, upstream = items
        latent, in_part, qkv_part, out_part = encode_object(feat_views, proj_views, live_count, upstream, in_weight, norm_gain, qkv_weight, out_weight)
        return ((running[0] + in_part, running[1] + qkv_part, running[2] + out_part), latent)
    start_sums = (jnp.zeros((FEAT, WIDTH), jnp.float32), jnp.zeros((WIDTH, 3 * WIDTH), jnp.float32), jnp.zeros((WIDTH, WIDTH), jnp.float32))
    sums, latent = lax.scan(advance, start_sums, (features, projection, active_count, cotangent))
    return (latent, sums[0], sums[1], sums[2])
```

```python
import jax
import jax.numpy as jnp
from jax import lax
from jax.experimental import pallas as pl
from jax.experimental.pallas import tpu as pltpu
from jax.sharding import PartitionSpec as P

HEAD_DIM = 64
F32 = jnp.float32
BF16 = jnp.bfloat16
VMEM_LIMIT = 60 * 1024 * 1024

NN = (((1,), (0,)), ((), ()))
NT = (((1,), (1,)), ((), ()))
TN = (((0,), (0,)), ((), ()))


def dot(lhs, rhs, dims):
    return lax.dot_general(lhs, rhs, dims, preferred_element_type=F32)


def vmem_call(body, out_shape, scalars, arrays, scratch=()):
    return pl.pallas_call(
        body,
        out_shape=out_shape,
        in_specs=[pl.BlockSpec(memory_space=pltpu.SMEM)] * len(scalars)
        + [pl.BlockSpec(memory_space=pltpu.VMEM)] * len(arrays),
        out_specs=jax.tree.map(lambda _: pl.BlockSpec(memory_space=pltpu.VMEM), out_shape),
        scratch_shapes=scratch,
        compiler_params=pltpu.CompilerParams(vmem_limit_bytes=VMEM_LIMIT),
    )(*scalars, *arrays)


def exchange(value, axis, mask):
    size = lax.axis_size(axis)
    return lax.ppermute(value, axis, [(i, i ^ mask) for i in range(size)])


def bit_masks(size):
    bits = size.bit_length() - 1
    masks = [1 << b for b in range(bits)]
    if bits >= 3:
        masks[2] = 6
    return masks


def keep_bit(index, masks, which):
    mask = masks[which]
    if mask == 2 and 6 in masks:
        return ((index >> 1) ^ (index >> 2)) & 1
    top = mask.bit_length() - 1
    return (index >> top) & 1


def totals_body(block, core_ref, proj_ref, feat_ref, own_ref, send_ref):
    core = core_ref[0]
    rows = own_ref.shape[0]
    row = lax.broadcasted_iota(jnp.int32, (rows, 1), 0)
    for half, ref in ((1 - core, send_ref), (core, own_ref)):
        ids = ((row // block) * 2 + half) * block + row % block
        onehot = jnp.where(proj_ref[...] == ids, 1.0, 0.0).astype(BF16)
        ref[...] = dot(onehot, feat_ref[...], NN).astype(ref.dtype)


def counts_body(block, core_ref, proj_ref, inv_ref):
    core = core_ref[0]
    rows = inv_ref.shape[0]
    row = lax.broadcasted_iota(jnp.int32, (rows, 1), 0)
    ids = ((row // block) * 2 + core) * block + row % block
    onehot = jnp.where(proj_ref[...] == ids, 1.0, 0.0)
    inv_ref[...] = jnp.maximum(jnp.sum(onehot, axis=1, keepdims=True), 1.0)


def attend_body(
    block, core_ref, active_ref, own_ref, other_ref, in_wt_ref, wt_ref, gain_ref, douts_ref,
    gp_ref, att_ref, unit_ref, inv_ref, normed_ref, vox_ref, packed_ref
):
    core = core_ref[0]
    half = own_ref.shape[0]
    slots = 2 * half
    heads_rows = att_ref.shape[0]
    heads = heads_rows // HEAD_DIM
    own_at = pl.multiple_of(core * half, half)
    other_at = pl.multiple_of((1 - core) * half, half)
    vox_ref[pl.ds(own_at, half), :] = own_ref[...]
    vox_ref[pl.ds(other_at, half), :] = other_ref[...]
    base = dot(in_wt_ref[...], vox_ref[...], NT)
    width = base.shape[0]
    center = jnp.sum(base, axis=0, keepdims=True) * (1.0 / width)
    shifted = base - center
    spread = jnp.sum(shifted * shifted, axis=0, keepdims=True) * (1.0 / width)
    inverse = lax.rsqrt(spread + 1e-06)
    unit = shifted * inverse
    inv_ref[...] = inverse
    unit_ref[...] = unit
    normed_ref[...] = (unit * gain_ref[...]).astype(BF16)
    packed_ref[...] = dot(wt_ref[...], normed_ref[...], NN).astype(BF16)
    row = lax.broadcasted_iota(jnp.int32, (slots, 1), 0)
    local = row % half
    ids = ((local // block) * 2 + row // half) * block + local % block
    live = ids < active_ref[0]

    @pl.loop(0, heads)
    def _(head):
        at = pl.multiple_of(head * HEAD_DIM, HEAD_DIM)
        query = packed_ref[pl.ds(at, HEAD_DIM), :] * BF16(HEAD_DIM**-0.5)
        key = packed_ref[pl.ds(heads_rows + at, HEAD_DIM), :]
        value = packed_ref[pl.ds(2 * heads_rows + at, HEAD_DIM), :]
        dout = douts_ref[pl.ds(at, HEAD_DIM), :]
        scores = jnp.where(live, dot(key, query, TN), -1e30)
        peak = jnp.max(scores, axis=0, keepdims=True)
        expo = jnp.exp(scores - peak)
        weights = expo * (1.0 / jnp.sum(expo, axis=0, keepdims=True))
        probs = weights.astype(BF16)
        mixed = dot(value, probs, NN)
        att_ref[pl.ds(at, HEAD_DIM), :] = mixed.astype(BF16)
        gp_ref[pl.ds(2 * heads_rows + at, HEAD_DIM), :] = dot(dout, probs, NT).astype(BF16)
        delta = jnp.sum(dout.astype(F32) * mixed, axis=0, keepdims=True)
        grad = (weights * (dot(value, dout, TN) - delta)).astype(BF16)
        grad_query = dot(key, grad, NN) * HEAD_DIM**-0.5
        gp_ref[pl.ds(at, HEAD_DIM), :] = grad_query.astype(BF16)
        gp_ref[pl.ds(heads_rows + at, HEAD_DIM), :] = dot(query, grad, NT).astype(BF16)


def write_pieces(value, scratch_ref, flips, keep_ref, send_ref):
    scratch_ref[...] = value
    rows = scratch_ref.shape[0] // 4
    for piece in range(4):
        source = pl.multiple_of((flips ^ piece) * rows, 8)
        block = scratch_ref[pl.ds(source, rows), :]
        ref = send_ref if piece >= 2 else keep_ref
        ref[piece % 2] = block.astype(ref.dtype)


def own_grads_body(
    share_ref, flip_ref, normed_ref, gp_ref, att_ref, seed_ref, keep_ref, send_ref, acc_ref
):
    rows = acc_ref.shape[0]
    normed = normed_ref[pl.ds(pl.multiple_of(share_ref[0] * rows, 16), rows), :]
    value = jnp.concatenate(
        [dot(normed, gp_ref[...], NT), dot(att_ref[...], seed_ref[...], NN)], axis=1
    )
    write_pieces(value, acc_ref, flip_ref[0], keep_ref, send_ref)


def in_grad_body(
    flip_ref, gp_own_ref, gp_other_ref, w_own_ref, w_other_ref, unit_ref, inv_ref, gain_ref,
    seed_ref, vox_ref, keep_ref, send_ref, acc_ref
):
    grad_normed = dot(w_own_ref[...], gp_own_ref[...], NN) + dot(
        w_other_ref[...], gp_other_ref[...], NN
    )
    unit = unit_ref[...]
    width = unit.shape[0]
    grad_unit = grad_normed * gain_ref[...]
    mean_one = jnp.sum(grad_unit, axis=0, keepdims=True) * (1.0 / width)
    mean_two = jnp.sum(grad_unit * unit, axis=0, keepdims=True) * (1.0 / width)
    branch = inv_ref[...] * (grad_unit - mean_one - unit * mean_two)
    grad_base = (seed_ref[...].astype(F32) + branch).astype(BF16)
    write_pieces(dot(vox_ref[...], grad_base, NT), acc_ref, flip_ref[0], keep_ref, send_ref)


def assemble_body(
    core_ref, fa_ref, fb_ref, fc_ref, a0, a1, a2, b0, b1, b2, c0, c1, c2,
    in_ref, qkv_ref, out_ref
):
    core = core_ref[0]
    width = out_ref.shape[1]
    part = width // 2
    rows = a0.shape[0]
    for flips, half, pieces in ((fa_ref[0], core, (a0, a1, a2)), (fb_ref[0], 1 - core, (b0, b1, b2))):
        first, second, rest = pieces
        for piece in range(4):
            source = (first, second)[piece] if piece < 2 else rest.at[piece - 2]
            block = source[...].astype(F32)
            to = pl.multiple_of((flips ^ piece) * rows, 8)
            for third in range(3):
                column = pl.multiple_of(third * width + half * part, 128)
                qkv_ref[pl.ds(to, rows), pl.ds(column, part)] = block[:, third * part : third * part + part]
            side = 0 if first is a0 else part
            out_ref[pl.ds(to, rows), side : side + part] = block[:, 3 * part :]
    rows = c0.shape[0]
    for piece in range(4):
        source = (c0, c1)[piece] if piece < 2 else c2.at[piece - 2]
        to = pl.multiple_of((fc_ref[0] ^ piece) * rows, 8)
        in_ref[pl.ds(to, rows), :] = source[...].astype(F32)


def reduce_steps(streams, masks):
    keeps, sends, orders = zip(*streams)
    count = len(streams)
    got = [exchange(s, "obj", masks[o[0]]) for s, o in zip(sends, orders)]
    halves = [k + g.astype(F32) for k, g in zip(keeps, got)]
    got = [exchange(h[1].astype(BF16), "obj", masks[o[1]]) for h, o in zip(halves, orders)]
    parts = [h[0] + g.astype(F32) for h, g in zip(halves, got)]
    for step in range(2, len(masks)):
        parts = [p.astype(BF16) for p in parts]
        got = [exchange(p, "obj", masks[o[step]]) for p, o in zip(parts, orders)]
        parts = [p.astype(F32) + g.astype(F32) for p, g in zip(parts, got)]
    parts = [p.astype(BF16) for p in parts]
    seconds = [exchange(p, "obj", masks[o[1]]) for p, o in zip(parts, orders)]
    rests = [
        exchange(jnp.stack([p, s]), "obj", masks[o[0]]) for p, s, o in zip(parts, seconds, orders)
    ]
    return [(parts[i], seconds[i], rests[i]) for i in range(count)]


def per_device(
    features, projection, active_count, in_weight, norm_gain, qkv_weight, out_weight, cotangent
):
    groups = lax.axis_size("view")
    objects = lax.axis_size("obj")
    view = lax.axis_index("view")
    obj = lax.axis_index("obj")
    core = view % 2
    core_s = core[None]
    block = cotangent.shape[1]
    slots = block * groups
    half = slots // 2
    feat = in_weight.shape[0]
    width = out_weight.shape[0]
    part = width // 2
    share = width // groups
    share_in = feat // groups

    rows = cotangent[0]
    mask = 2
    stack = rows[None]
    while mask < groups:
        got = exchange(stack, "view", mask)
        low = (view & mask) == 0
        stack = jnp.concatenate([jnp.where(low, stack, got), jnp.where(low, got, stack)])
        mask *= 2
    rows = stack.reshape(half, width)
    got = exchange(rows, "view", 1)
    cot = jnp.concatenate([jnp.where(core == 0, rows, got), jnp.where(core == 0, got, rows)])
    slot = lax.iota(jnp.int32, slots)
    slot_ids = ((slot % half // block) * 2 + slot // half) * block + slot % block
    live = (slot_ids < active_count[0]).astype(F32)
    seed = (cot.astype(F32) * live[:, None] * (1.0 / objects)).astype(BF16)
    seed_t = seed.T

    local_feat = features.reshape(features.shape[1] * features.shape[2], feat)
    flat_proj = projection.reshape(1, projection.shape[1] * projection.shape[2])
    local_rows = local_feat.shape[0]
    own_proj = lax.dynamic_slice_in_dim(flat_proj, view * local_rows, local_rows, 1)
    own, send = vmem_call(
        lambda *refs: totals_body(block, *refs),
        (jax.ShapeDtypeStruct((half, feat), F32), jax.ShapeDtypeStruct((half, feat), BF16)),
        (core_s,),
        (own_proj, local_feat),
    )
    total = own + exchange(send, "view", 1).astype(F32)
    mask = 2
    while mask < groups:
        total = total + exchange(total.astype(BF16), "view", mask).astype(F32)
        mask *= 2
    counts = vmem_call(
        lambda *refs: counts_body(block, *refs),
        jax.ShapeDtypeStruct((half, 1), F32),
        (core_s,),
        (flat_proj,),
    )
    vox_own = (total / counts).astype(BF16)
    vox_other = exchange(vox_own, "view", 1)

    def columns(which):
        return jnp.concatenate(
            [
                lax.dynamic_slice_in_dim(qkv_weight, t * width + which * part, part, 1)
                for t in range(3)
            ],
            axis=1,
        )

    w_own, w_other = columns(core), columns(1 - core)
    out_rows = lax.dynamic_slice_in_dim(out_weight, core * part, part, 0)
    douts = dot(out_rows, seed, NT).astype(BF16)
    gain = norm_gain[:, None]

    gp_own, att_own, unit, inverse, normed = vmem_call(
        lambda *refs: attend_body(block, *refs),
        (
            jax.ShapeDtypeStruct((3 * part, slots), BF16),
            jax.ShapeDtypeStruct((part, slots), BF16),
            jax.ShapeDtypeStruct((width, slots), F32),
            jax.ShapeDtypeStruct((1, slots), F32),
            jax.ShapeDtypeStruct((width, slots), BF16),
        ),
        (core_s, active_count),
        (vox_own, vox_other, in_weight.T, w_own.T, gain, douts),
        [pltpu.VMEM((slots, feat), BF16), pltpu.VMEM((3 * part, slots), BF16)],
    )
    att_other = exchange(att_own, "view", 1)
    gp_other = exchange(gp_own, "view", 1)

    masks = bit_masks(objects)
    orders = [[(s + j) % len(masks) for j in range(len(masks))] for s in (0, 1, 2)]
    flips = [
        (keep_bit(obj, masks, o[0]) * 2 + keep_bit(obj, masks, o[1])).astype(jnp.int32)[None]
        for o in orders
    ]
    att = jnp.where(core == 0, jnp.stack([att_own, att_other]), jnp.stack([att_other, att_own]))
    att_share = lax.dynamic_slice_in_dim(att.reshape(width, slots), view * share, share, 0)
    vox = jnp.where(core == 0, jnp.stack([vox_own, vox_other]), jnp.stack([vox_other, vox_own]))
    vox_share = lax.dynamic_slice_in_dim(vox.reshape(slots, feat), view * share_in, share_in, 1).T

    def pieces(r, c):
        return (
            jax.ShapeDtypeStruct((2, r // 4, c), F32),
            jax.ShapeDtypeStruct((2, r // 4, c), BF16),
        )

    def half_grads(gp, seed_cols, flip):
        return vmem_call(
            own_grads_body,
            pieces(share, 2 * width),
            (view[None], flip),
            (normed, gp, att_share, seed_cols),
            [pltpu.VMEM((share, 2 * width), F32)],
        )

    first = half_grads(gp_own, seed[:, :part], flips[0])
    second = half_grads(gp_other, seed[:, part:], flips[1])
    third = vmem_call(
        in_grad_body,
        pieces(share_in, width),
        (flips[2],),
        (gp_own, gp_other, w_own, w_other, unit, inverse, gain, seed_t, vox_share),
        [pltpu.VMEM((share_in, width), F32)],
    )
    sums = reduce_steps(
        [(*first, orders[0]), (*second, orders[1]), (*third, orders[2])], masks
    )
    in_grad, qkv_grad, out_grad = vmem_call(
        assemble_body,
        (
            jax.ShapeDtypeStruct((share_in, width), F32),
            jax.ShapeDtypeStruct((share, 3 * width), F32),
            jax.ShapeDtypeStruct((share, width), F32),
        ),
        (core_s, *flips),
        tuple(x for s in sums for x in s),
    )

    chip = view // 2
    vox_rows = lax.dynamic_slice_in_dim(vox_own, chip * block, block, 0)
    att_cols = lax.dynamic_slice_in_dim(
        att.reshape(width, slots), core * half + chip * block, block, 1
    )
    latent = dot(vox_rows, in_weight, NN) + dot(att_cols, out_weight, TN)
    own_ids = view * block + lax.iota(jnp.int32, block)
    live_rows = (own_ids < active_count[0]).astype(F32)
    latent = (live_rows[:, None] * latent).astype(BF16)
    return (latent[None], in_grad, qkv_grad, out_grad)


def solution(mesh):
    return jax.shard_map(
        per_device,
        mesh=mesh,
        in_specs=(
            P("obj", "view", None, None),
            P("obj", None, None),
            P("obj"),
            P(),
            P(),
            P(),
            P(),
            P("obj", "view", None),
        ),
        out_specs=(P("obj", "view", None), P("view", None), P("view", None), P("view", None)),
        check_vma=False,
    )
```

```python
import jax
import jax.numpy as jnp
from jax import lax
from jax.experimental import pallas as pl
from jax.experimental.pallas import tpu as pltpu
from jax.sharding import PartitionSpec as P


HEAD_DIM = 64
F32 = jnp.float32
BF16 = jnp.bfloat16
UNROLL = 6
CHUNKS = 1
ORDERS = "mmm"
SPARE = 2 * 1024 * 1024

NN = (((1,), (0,)), ((), ()))
NT = (((1,), (1,)), ((), ()))
TN = (((0,), (0,)), ((), ()))


def dot(lhs, rhs, dims):
    return lax.dot_general(lhs, rhs, dims, preferred_element_type=F32)


def size_of(shape, dtype):
    rows = -(-shape[-2] // 16) * 16 if len(shape) > 1 else 8
    lanes = -(-shape[-1] // 128) * 128
    lead = 1
    for extent in shape[:-2]:
        lead *= extent
    return lead * rows * lanes * jnp.dtype(dtype).itemsize


def vmem_call(body, out_shape, scalars, arrays, scratch=(), temps=0, **kwargs):
    outs = jax.tree.leaves(out_shape)
    limit = SPARE + temps + sum(size_of(a.shape, a.dtype) for a in (*arrays, *outs, *scratch))
    vmem = pl.BlockSpec(memory_space=pltpu.VMEM)
    specs = dict(
        in_specs=[pl.BlockSpec(memory_space=pltpu.SMEM)] * len(scalars) + [vmem] * len(arrays),
        out_specs=jax.tree.map(lambda _: vmem, out_shape),
    )
    specs.update(kwargs)
    return pl.pallas_call(
        body,
        out_shape=out_shape,
        scratch_shapes=[pltpu.VMEM(s.shape, s.dtype) for s in scratch],
        compiler_params=pltpu.CompilerParams(vmem_limit_bytes=limit),
        **specs,
    )(*scalars, *arrays)


def shape(dims, dtype):
    return jax.ShapeDtypeStruct(dims, dtype)


def exchange(value, axis, mask):
    size = lax.axis_size(axis)
    return lax.ppermute(value, axis, [(i, i ^ mask) for i in range(size)])


def exchange_obj(value, masks):
    objects, groups = lax.axis_size("obj"), lax.axis_size("view")
    pairs = [
        (o * groups + v, (o ^ masks[v % 2]) * groups + v)
        for o in range(objects)
        for v in range(groups)
    ]
    return lax.ppermute(value, ("obj", "view"), pairs)


def aligned(value, multiple):
    return pl.multiple_of(value, multiple)


def totals_body(block, place_ref, proj_ref, feat_ref, own_ref, send_ref, onehot_ref):
    view, core = place_ref[0], place_ref[1]
    rows = own_ref.shape[0]
    locals_, _ = feat_ref.shape[1:3]

    @pl.when(pl.program_id(0) == 0)
    def _():
        row = lax.broadcasted_iota(jnp.int32, (2 * rows, 1), 0)
        half = jnp.where(row < rows, 1 - core, core)
        row = row % rows
        ids = ((row // block) * 2 + half) * block + row % block
        for local in range(locals_):
            proj = proj_ref[0, pl.ds(view * locals_ + local, 1), :]
            onehot_ref[local] = jnp.where(proj == ids, 1.0, 0.0).astype(BF16)

    sums = dot(onehot_ref[0], feat_ref[0, 0], NN)
    for local in range(1, locals_):
        sums += dot(onehot_ref[local], feat_ref[0, local], NN)
    send_ref[...] = sums[:rows].astype(BF16)
    own_ref[...] = sums[rows:]


def counts_body(block, place_ref, proj_ref, count_ref):
    core = place_ref[1]
    half = count_ref.shape[0]
    low = 16
    high = 2 * half // low
    table = jnp.zeros((high, low), F32)
    for v in range(proj_ref.shape[1]):
        proj = proj_ref[0, pl.ds(v, 1), :]
        tall = lax.broadcasted_iota(jnp.int32, (high, 1), 0) == proj // low
        flat = lax.broadcasted_iota(jnp.int32, (low, 1), 0) == proj % low
        table += dot(
            jnp.where(tall, 1.0, 0.0).astype(BF16), jnp.where(flat, 1.0, 0.0).astype(BF16), NT
        )
    row = lax.broadcasted_iota(jnp.int32, (half, 1), 0)
    ids = ((row // block) * 2 + core) * block + row % block
    pick = jnp.where(lax.broadcasted_iota(jnp.int32, (1, high), 1) == ids // low, 1.0, 0.0)
    lines = lax.dot_general(pick, table, NN, precision=lax.Precision.HIGHEST)
    here = lax.broadcasted_iota(jnp.int32, (1, low), 1) == ids % low
    counts = jnp.sum(jnp.where(here, lines, 0.0), axis=1, keepdims=True)
    count_ref[...] = jnp.maximum(counts, 1.0)


def base_body(own_ref, got_ref, counts_ref, in_ref, mean_ref, mean_send_ref, base_ref, send_ref):
    mean = (own_ref[...] + got_ref[...].astype(F32)) * (1.0 / counts_ref[...])
    mean_ref[...] = mean
    rounded = mean.astype(BF16)
    mean_send_ref[...] = rounded
    base = dot(rounded, in_ref[...], NN)
    base_ref[...] = base
    send_ref[...] = base.astype(BF16)


def add_body(own_ref, got_ref, total_ref, send_ref):
    total = own_ref[...] + got_ref[...].astype(F32)
    total_ref[...] = total
    send_ref[...] = total.astype(BF16)


def norm_body(part_ref, got_ref, gain_ref, base_ref, packet_ref):
    base = part_ref[...] + got_ref[...].astype(F32)
    base_ref[...] = base
    width = base.shape[1]
    shifted = base - jnp.sum(base, axis=1, keepdims=True) * (1.0 / width)
    spread = jnp.sum(shifted * shifted, axis=1, keepdims=True) * (1.0 / width)
    inverse = lax.rsqrt(spread + 1e-06)
    packet_ref[:, :width] = (shifted * inverse * gain_ref[...]).astype(BF16)
    lane = lax.broadcasted_iota(jnp.int32, (1, packet_ref.shape[1] - width), 1)
    rest = inverse
    tail = jnp.zeros((base.shape[0], packet_ref.shape[1] - width), F32)
    for digit in range(3):
        rounded = rest.astype(BF16).astype(F32)
        tail = jnp.where(lane == digit, rounded, tail)
        rest = rest - rounded
    packet_ref[:, width:] = tail.astype(BF16)


def voxel_body(place_ref, mean_ref, got_ref, keep_ref, send_ref):
    share = keep_ref.shape[0]
    for ref, view in ((keep_ref, place_ref[0]), (send_ref, place_ref[0] ^ 1)):
        lanes = pl.ds(aligned(view * share, 128), share)
        ref[...] = (mean_ref[:, lanes] + got_ref[:, lanes].astype(F32)).astype(BF16).T


def halve_body(keep_ref, got_ref, kept_ref, send_ref):
    kept_ref[...] = keep_ref[0] + got_ref[0].astype(F32)
    send_ref[...] = (keep_ref[1] + got_ref[1].astype(F32)).astype(BF16)


def stack_body(first_ref, second_ref, pair_ref):
    pair_ref[0] = first_ref[...]
    pair_ref[1] = second_ref[...]


def sum_body(kept_ref, got_ref, sum_ref):
    sum_ref[...] = (kept_ref[...].astype(F32) + got_ref[...].astype(F32)).astype(BF16)


def prepare_body(
    block, bases, scale, place_ref, active_ref, qkv_ref, out_ref, gain_ref, *refs
):
    pieces = refs[: 2 * len(bases)]
    w_t_ref, douts_ref, seed_ref, seed_t_ref, gain_col_ref = refs[2 * len(bases) :]
    view, core = place_ref[0], place_ref[1]
    chip = view // 2
    active = active_ref[0]
    slots, width = seed_ref.shape
    half = slots // 2
    part = width // 2
    row = lax.broadcasted_iota(jnp.int32, (block, 1), 0)
    for number, piece in enumerate(pieces):
        side = core if number < len(bases) else 1 - core
        for i in range(piece.shape[0]):
            place = chip ^ (bases[number % len(bases)] + i)
            live = jnp.where((place * 2 + side) * block + row < active, scale, 0.0)
            at = aligned(side * half + place * block, block)
            seed_ref[pl.ds(at, block), :] = (piece[i].astype(F32) * live).astype(BF16)
    seed = seed_ref[...]
    seed_t_ref[...] = seed.T
    douts_ref[...] = dot(out_ref[pl.ds(aligned(core * part, part), part), :], seed, NT).astype(BF16)
    for third in range(3):
        at = aligned(third * width + core * part, 128)
        w_t_ref[pl.ds(third * part, part), :] = qkv_ref[:, pl.ds(at, part)].T
    gain_col_ref[...] = jnp.broadcast_to(gain_ref[...], (8, width)).T[:, :1]


def attend_body(
    block, place_ref, active_ref, own_ref, other_ref, wt_ref, douts_ref,
    gp_ref, att_ref, inv_ref, normed_ref, rows_ref, packed_ref
):
    core = place_ref[1]
    half = own_ref.shape[0]
    slots = 2 * half
    width = normed_ref.shape[0]
    heads_rows = att_ref.shape[0]
    heads = heads_rows // HEAD_DIM
    rows_ref[pl.ds(aligned(core * half, half), half), :] = own_ref[...]
    rows_ref[pl.ds(aligned((1 - core) * half, half), half), :] = other_ref[...]
    packed_ref[...] = dot(wt_ref[...], rows_ref[:, :width], NT).astype(BF16)
    normed_ref[...] = rows_ref[:, :width].T
    tail = rows_ref[:, width:].astype(F32).T
    inv_ref[...] = tail[0:1] + tail[1:2] + tail[2:3]
    row = lax.broadcasted_iota(jnp.int32, (slots, 1), 0)
    local = row % half
    ids = ((local // block) * 2 + row // half) * block + local % block
    live = ids < active_ref[0]

    @pl.loop(0, heads, unroll=UNROLL)
    def _(head):
        at = aligned(head * HEAD_DIM, HEAD_DIM)
        key = packed_ref[pl.ds(heads_rows + at, HEAD_DIM), :]
        value = packed_ref[pl.ds(2 * heads_rows + at, HEAD_DIM), :]
        grad_key = grad_value = None
        for chunk in range(CHUNKS):
            lanes = slice(chunk * slots // CHUNKS, (chunk + 1) * slots // CHUNKS)
            query = packed_ref[pl.ds(at, HEAD_DIM), lanes] * BF16(HEAD_DIM**-0.5)
            dout = douts_ref[pl.ds(at, HEAD_DIM), lanes]
            scores = jnp.where(live, dot(key, query, TN), -1e30)
            peak = jnp.max(scores, axis=0, keepdims=True)
            expo = jnp.exp(scores - peak)
            weights = expo * (1.0 / jnp.sum(expo, axis=0, keepdims=True))
            probs = weights.astype(BF16)
            mixed = dot(value, probs, NN)
            att_ref[pl.ds(at, HEAD_DIM), lanes] = mixed.astype(BF16)
            value_piece = dot(dout, probs, NT)
            delta = jnp.sum(dout.astype(F32) * mixed, axis=0, keepdims=True)
            grad = (weights * (dot(value, dout, TN) - delta)).astype(BF16)
            grad_query = dot(key, grad, NN) * HEAD_DIM**-0.5
            gp_ref[pl.ds(at, HEAD_DIM), lanes] = grad_query.astype(BF16)
            key_piece = dot(query, grad, NT)
            grad_key = key_piece if grad_key is None else grad_key + key_piece
            grad_value = value_piece if grad_value is None else grad_value + value_piece
        gp_ref[pl.ds(heads_rows + at, HEAD_DIM), :] = grad_key.astype(BF16)
        gp_ref[pl.ds(2 * heads_rows + at, HEAD_DIM), :] = grad_value.astype(BF16)


def split_rows(value, flips, keep_ref, send_ref):
    def swapped(flip, pair):
        low, high = pair
        return jnp.where(flip == 0, low, high), jnp.where(flip == 0, high, low)

    def halves(rows):
        count = rows.shape[0] // 2
        return rows[:count], rows[count:]

    keep, send = swapped(flips[0], halves(value))
    keep_ref[0], keep_ref[1] = swapped(flips[1], halves(keep))
    first, second = swapped(flips[1], halves(send))
    send_ref[0], send_ref[1] = first.astype(BF16), second.astype(BF16)


def qkv_grads_body(flips, place_ref, normed_ref, gp_ref, keep_ref, send_ref):
    rows = 4 * keep_ref.shape[1]
    normed = normed_ref[pl.ds(aligned(place_ref[0] * rows, 16), rows), :]
    split_rows(dot(normed, gp_ref[...], NT), flips(place_ref, 0), keep_ref, send_ref)


def qkv_out_grads_body(
    flips, place_ref, normed_ref, gp_ref, att_own_ref, att_other_ref, seed_ref, keep_ref, send_ref
):
    view, core = place_ref[0], place_ref[1]
    part = att_own_ref.shape[0]
    rows = 4 * keep_ref.shape[1]
    first = view * rows
    normed = normed_ref[pl.ds(aligned(first, 16), rows), :]
    local = pl.ds(aligned(first % part, 16), rows)
    att = jnp.where(first // part == core, att_own_ref[local, :], att_other_ref[local, :])
    value = jnp.concatenate([dot(normed, gp_ref[...], NT), dot(att, seed_ref[...], NN)], axis=1)
    split_rows(value, flips(place_ref, 1), keep_ref, send_ref)


def head_columns(qkv_ref, which, width):
    part = width // 2
    return [qkv_ref[:, pl.ds(aligned(t * width + which * part, 128), part)] for t in range(3)]


def own_branch_body(place_ref, qkv_ref, gp_ref, grad_ref):
    width = grad_ref.shape[0]
    part = width // 2
    weights = head_columns(qkv_ref, place_ref[1], width)
    grad_ref[...] = sum(dot(w, gp_ref[t * part : t * part + part], NN) for t, w in enumerate(weights))


def in_grad_body(
    flips, place_ref, qkv_ref, gp_ref, grad_ref, normed_ref, inv_ref, gain_ref, seed_ref, own_ref,
    other_ref,    keep_ref, send_ref
):
    width = normed_ref.shape[0]
    part = width // 2
    weights = head_columns(qkv_ref, 1 - place_ref[1], width)
    grad_normed = grad_ref[...] + sum(
        dot(w, gp_ref[t * part : t * part + part], NN) for t, w in enumerate(weights)
    )
    unit = normed_ref[...].astype(F32) * (1.0 / gain_ref[...])
    grad_unit = grad_normed * gain_ref[...]
    mean_one = jnp.sum(grad_unit, axis=0, keepdims=True) * (1.0 / width)
    mean_two = jnp.sum(grad_unit * unit, axis=0, keepdims=True) * (1.0 / width)
    branch = inv_ref[...] * (grad_unit - mean_one - unit * mean_two)
    grad_base = (seed_ref[...].astype(F32) + branch).astype(BF16)
    own, other = own_ref[...], other_ref[...]
    half = own.shape[1]
    first = jnp.where(place_ref[1] == 0, own, other)
    second = jnp.where(place_ref[1] == 0, other, own)
    value = dot(first, grad_base[:, :half], NT) + dot(second, grad_base[:, half:], NT)
    split_rows(value, flips(place_ref, 2), keep_ref, send_ref)


def latent_body(
    block, place_ref, active_ref, base_ref, att_own_ref, att_other_ref, out_ref, latent_ref
):
    view, core = place_ref[0], place_ref[1]
    chip = view // 2
    half = base_ref.shape[0]
    part = att_own_ref.shape[0]
    value = base_ref[pl.ds(aligned(chip * block, block), block), :]
    lanes = pl.ds(aligned(core * half + chip * block, block), block)
    for ref, which in ((att_own_ref, core), (att_other_ref, 1 - core)):
        value += dot(ref[:, lanes], out_ref[pl.ds(aligned(which * part, part), part), :], TN)
    row = lax.broadcasted_iota(jnp.int32, (block, 1), 0)
    live = jnp.where(view * block + row < active_ref[0], 1.0, 0.0)
    latent_ref[...] = (live * value).astype(BF16)


def placed(flips, place_ref, side, pairs):
    high, low = flips(place_ref, side)
    rows = pairs[0].shape[1]
    for piece in range(4):
        to = aligned(((high * 2 + low) ^ piece) * rows, 8)
        yield pl.ds(to, rows), pairs[piece // 2][piece % 2].astype(F32)


def assemble_body(flips, place_ref, a0, a1, b0, b1, qkv_ref, out_ref):
    core = place_ref[1]
    width = out_ref.shape[1]
    part = width // 2
    for side, half, pairs in ((0, core, (a0, a1)), (1, 1 - core, (b0, b1))):
        for to, block in placed(flips, place_ref, side, pairs):
            for third in range(3):
                column = aligned(third * width + half * part, 128)
                qkv_ref[to, pl.ds(column, part)] = block[:, third * part : third * part + part]
            if side == 1:
                out_ref[to, :] = block[:, 3 * part :]


def assemble_in_body(flips, place_ref, c0, c1, in_ref):
    for to, block in placed(flips, place_ref, 2, (c0, c1)):
        in_ref[to, :] = block


def reduce_steps(streams, orders, later):
    sides = range(3)

    def swap(values, turn):
        got = []
        for side in sides:
            got.append(exchange_obj(values[side], turn(side)))
        return got

    def call(body, outs, *arrays):
        results = []
        for side in sides:
            results.append(vmem_call(body, outs(side), (), tuple(a[side] for a in arrays)))
        return results

    keeps, sends = zip(*streams)
    got = swap(sends, lambda side: orders[side][0])

    def piece(dtype):
        return lambda side: shape(keeps[side].shape[1:], dtype)

    kept, sends = zip(
        *call(halve_body, lambda side: (piece(F32)(side), piece(BF16)(side)), keeps, got)
    )
    got = swap(sends, lambda side: orders[side][1])
    kept = call(sum_body, piece(BF16), kept, got)
    for mask in later:
        got = swap(kept, lambda side: (mask, mask))
        kept = call(sum_body, piece(BF16), kept, got)
    got = swap(kept, lambda side: orders[side][1])
    pairs = call(stack_body, lambda side: shape(keeps[side].shape, BF16), kept, got)
    rests = swap(pairs, lambda side: orders[side][0])
    return [x for pair in zip(pairs, rests) for x in pair]


def per_device(
    features, projection, active_count, in_weight, norm_gain, qkv_weight, out_weight, cotangent
):
    groups = lax.axis_size("view")
    objects = lax.axis_size("obj")
    view = lax.axis_index("view")
    obj = lax.axis_index("obj")
    core = view % 2
    place = jnp.stack([view, core, obj])
    block = cotangent.shape[1]
    slots = block * groups
    half = slots // 2
    feat = in_weight.shape[0]
    width = out_weight.shape[0]
    part = width // 2
    share = width // groups
    share_in = feat // groups

    tile = 512
    views, patches = features.shape[1:3]
    own, send = vmem_call(
        lambda *refs: totals_body(block, *refs),
        (shape((half, feat), F32), shape((half, feat), BF16)),
        (place,),
        tuple(pltpu.with_memory_space_constraint(x, pltpu.HBM) for x in (projection, features)),
        [shape((views, slots, patches), BF16)],
        grid=(feat // tile,),
        in_specs=[
            pl.BlockSpec(memory_space=pltpu.SMEM),
            pl.BlockSpec(projection.shape, lambda i: (0, 0, 0)),
            pl.BlockSpec((1, views, patches, tile), lambda i: (0, 0, 0, i)),
        ],
        out_specs=[pl.BlockSpec((half, tile), lambda i: (0, i))] * 2,
    )

    pieces = [cotangent]
    mask = 2
    while mask < groups:
        pieces.append(exchange(jnp.concatenate(pieces), "view", mask))
        mask *= 2
    bases = [sum(p.shape[0] for p in pieces[:i]) for i in range(len(pieces))]
    pieces += [exchange(p, "view", 1) for p in pieces]

    got = exchange(send, "view", 1)
    counts = vmem_call(
        lambda *refs: counts_body(block, *refs),
        shape((half, 1), F32),
        (place,),
        (projection,),
    )
    mean, mean_send, base, send = vmem_call(
        base_body,
        (
            shape((half, feat), F32),
            shape((half, feat), BF16),
            shape((half, width), F32),
            shape((half, width), BF16),
        ),
        (),
        (own, got, counts, in_weight),
        temps=4 * half * feat,
    )

    def chip_sums(value, send):
        got = exchange(send, "view", 2)
        mask = 4
        while mask < groups:
            value, send = vmem_call(
                add_body, (shape(value.shape, F32), shape(value.shape, BF16)), (), (value, got)
            )
            got = exchange(send, "view", mask)
            mask *= 2
        return value, got

    base, base_got = chip_sums(base, send)
    mean, mean_got = chip_sums(mean, mean_send)
    w_t, douts, seed, seed_t, gain = vmem_call(
        lambda *refs: prepare_body(block, bases, 1.0 / objects, *refs),
        (
            shape((3 * part, width), BF16),
            shape((part, slots), BF16),
            shape((slots, width), BF16),
            shape((width, slots), BF16),
            shape((width, 1), F32),
        ),
        (place, active_count),
        (qkv_weight, out_weight, norm_gain[None], *pieces),
        temps=4 * slots * width,
    )
    base_own, packet = vmem_call(
        norm_body,
        (shape((half, width), F32), shape((half, width + 128), BF16)),
        (),
        (base, base_got, norm_gain[None]),
        temps=8 * half * width,
    )
    packet_other = exchange(packet, "view", 1)
    gp_own, att_own, inverse, normed = vmem_call(
        lambda *refs: attend_body(block, *refs),
        (
            shape((3 * part, slots), BF16),
            shape((part, slots), BF16),
            shape((1, slots), F32),
            shape((width, slots), BF16),
        ),
        (place, active_count),
        (packet, packet_other, w_t, douts),
        [shape((slots, width + 128), BF16), shape((3 * part, slots), BF16)],
        temps=24 * slots * slots,
    )
    vox_own, vox_send = vmem_call(
        voxel_body,
        (shape((share_in, half), BF16), shape((share_in, half), BF16)),
        (place,),
        (mean, mean_got),
    )
    vox_other = exchange(vox_send, "view", 1)
    att_other = exchange(att_own, "view", 1)
    gp_other = exchange(gp_own, "view", 1)

    both, across, along = ((1, 2), (2, 1)), ((1, 1), (2, 2)), ((2, 2), (1, 1))
    orders = [{"m": both, "x": across, "z": along}[kind] for kind in ORDERS]
    later = [1 << bit for bit in range(2, objects.bit_length() - 1)]

    def flips(place_ref, side):
        def bit(masks):
            low, high = ((place_ref[2] >> (m - 1)) & 1 for m in masks)
            return jnp.where(place_ref[1] == 0, low, high)

        return [bit(masks) for masks in orders[side]]

    def halves(r, c):
        return (shape((2, r // 4, c), F32), shape((2, r // 4, c), BF16))

    grad_own = vmem_call(
        own_branch_body,
        shape((width, slots), F32),
        (place,),
        (qkv_weight, gp_own),
        temps=4 * slots * width,
    )
    streams = [None] * 3
    streams[0] = vmem_call(
        lambda *refs: qkv_grads_body(flips, *refs),
        halves(share, 3 * part),
        (place,),
        (normed, gp_own),
        temps=8 * share * width,
    )
    streams[1] = vmem_call(
        lambda *refs: qkv_out_grads_body(flips, *refs),
        halves(share, 3 * part + width),
        (place,),
        (normed, gp_other, att_own, att_other, seed),
        temps=8 * share * width,
    )
    streams[2] = vmem_call(
        lambda *refs: in_grad_body(flips, *refs),
        halves(share_in, width),
        (place,),
        (qkv_weight, gp_other, grad_own, normed, inverse, gain, seed_t, vox_own, vox_other),
        temps=8 * slots * width,
    )
    sums = reduce_steps(streams, orders, later)
    qkv_grad, out_grad = vmem_call(
        lambda *refs: assemble_body(flips, *refs),
        (shape((share, 3 * width), F32), shape((share, width), F32)),
        (place,),
        sums[:4],
    )
    in_grad = vmem_call(
        lambda *refs: assemble_in_body(flips, *refs),
        shape((share_in, width), F32),
        (place,),
        sums[4:],
    )
    latent = vmem_call(
        lambda *refs: latent_body(block, *refs),
        shape((block, width), BF16),
        (place, active_count),
        (base_own, att_own, att_other, out_weight),
    )
    return (latent[None], in_grad, qkv_grad, out_grad)


def solution(mesh):
    return jax.shard_map(
        per_device,
        mesh=mesh,
        in_specs=(
            P("obj", "view", None, None),
            P("obj", None, None),
            P("obj"),
            P(),
            P(),
            P(),
            P(),
            P("obj", "view", None),
        ),
        out_specs=(P("obj", "view", None), P("view", None), P("view", None), P("view", None)),
        check_vma=False,
    )
```
